32 devices in a mesh: rows: 16 (over z, y, core), cols: 2 (over x).
Axes of the slice: x: 2, y: 2, z: 4, core: 2. Of those that a mesh axis runs over, the one named last changes fastest.
Arguments:
- design: bfloat16 [32768, 6144], P('rows', 'cols'), may hold values from -0.03125 to 0.03125
- targets: bfloat16 [32768, 128], P('rows'), may hold values from -6 to 6
- col_scale: float32 [6144], P('cols'), may hold values from 0.1 to 1
Outputs:
- solution: float32 [6144, 128], P('cols', 'rows')
- residual: float32 [32768, 128], P('rows')
The draws below stay inside these ranges and needn't reach their ends.
All inputs are finite; a program needn't handle non-finite values.
Results may differ from the reference program's by a relative error of at most 0.0065.
Values may be sent and summed in bfloat16 or wider, within the bound.
A program may use at most 128 MiB of HBM per device.

```python
import math
import jax
import jax.numpy as jnp
from jax import lax

P_SIZE = 6144
FITS = 128
ITERS = 6
M = 32768


def levels(key, shape, cuts, low, high):
    def one(axis_at, shards_of):
        draws = jax.random.uniform(jax.random.fold_in(jax.random.fold_in(key, 6), axis_at), (shards_of,), jnp.float32, low / len(cuts), high / len(cuts))
        return jnp.repeat(jnp.exp(draws), shape[axis_at] // shards_of).reshape((-1,) + (1,) * (len(shape) - axis_at - 1))

    level = one(*cuts[0])
    for cut in cuts[1:]:
        level = level * one(*cut)
    return level


def gaussian(own_key, extent, width, bound, pieces=(), held_as=jnp.bfloat16):
    gain = levels(own_key, extent, pieces, -0.22, 0.18) if pieces else 1.0
    values = jax.random.normal(own_key, extent, jnp.float32) * width * gain
    return jnp.minimum(jnp.maximum(values, -bound), bound).astype(held_as)


def setup_inputs(seed: int = 0) -> dict:
    seeds = jax.random.split(jax.random.key(seed), 4)
    design = gaussian(seeds[0], (M, P_SIZE), M ** -0.5, 0.03125, ((0, 16), (1, 2)))
    targets = gaussian(seeds[1], (M, FITS), 1.0, 6.0, ((0, 16),))
    col_scale = jnp.clip(jnp.exp(math.log(1.0) - 2.3025851 * jax.random.uniform(seeds[2], (P_SIZE,), jnp.float32) ** levels(seeds[2], (P_SIZE,), ((0, 2),), -0.2, 0.2)), 0.1, 1.0)
    return dict(design=design, targets=targets, col_scale=col_scale)


def back_apply(design, scale, vectors):
    product = lax.dot_general(design, vectors, (((0,), (0,)), ((), ())), preferred_element_type=jnp.float32)
    return scale * product


def reference(design, targets, col_scale):
    scale = col_scale[:, None]
    gradient = back_apply(design, scale, targets)
    gamma = jnp.sum(gradient * gradient, axis=0)
    solution = jnp.zeros(gradient.shape, jnp.float32)
    residual = targets.astype(jnp.float32)
    direction = gradient
    for step in range(ITERS):
        scaled_dir = (scale * direction).astype(jnp.bfloat16)
        image = jnp.dot(design, scaled_dir, preferred_element_type=jnp.float32)
        delta = jnp.sum(image * image, axis=0)
        alpha = gamma / delta
        solution = solution + alpha * direction
        residual = residual - alpha * image
        if step + 1 < ITERS:
            gradient = back_apply(design, scale, residual.astype(jnp.bfloat16))
            gamma_new = jnp.sum(gradient * gradient, axis=0)
            direction = gradient + (gamma_new / gamma) * direction
            gamma = gamma_new
    return solution, residual
```

```python
import functools

import jax
import jax.numpy as jnp
from jax import lax
from jax.experimental import pallas as pl
from jax.experimental.pallas import tpu as pltpu
from jax.sharding import PartitionSpec as P

ITERS = 6
BLOCKS = 4
F32 = jnp.float32
BF16 = jnp.bfloat16
MESH = pl.DeviceIdType.MESH


def kernel(n, design_hbm, targets_ref, scale_ref, sol_ref, res_ref,
           design, h_ref, img, spm, sp_all, xs, xr, cs, cr, rs, rr, st, gx,
           g_ref, p_ref, gam_ref,
           load_sem, x_send, x_recv, c_send, c_recv, r_send, r_recv,
           a_send, a_recv, f_send, s_send, s_recv, g_send, g_recv):
    rows, width = design.shape
    fits = targets_ref.shape[1]
    own = fits // n
    chips = n // 2
    block = rows // BLOCKS
    wide = 512 if width % 512 == 0 else width
    r, c = lax.axis_index("rows"), lax.axis_index("cols")
    core, chip = lax.rem(r, 2), lax.div(r, 2)
    sibling = r + 1 - 2 * core
    partner = (r, 1 - c)

    def remote(src, dst, send, recv, to):
        return pltpu.make_async_remote_copy(
            src_ref=src, dst_ref=dst, send_sem=send, recv_sem=recv,
            device_id=to, device_id_type=MESH)

    def load(b):
        at = pl.ds(b * block, block)
        return pltpu.make_async_copy(design_hbm.at[at], design.at[at], load_sem.at[b])

    for b in range(BLOCKS):
        load(b).start()
    barrier = pltpu.get_barrier_semaphore()

    @pl.loop(1, n)
    def _(d):
        pl.semaphore_signal(barrier, inc=1, device_id=(lax.rem(r + d, n), c), device_id_type=MESH)

    pl.semaphore_signal(barrier, inc=1, device_id=partner, device_id_type=MESH)

    lane = lax.broadcasted_iota(jnp.int32, (own, fits), 1)
    row = lax.broadcasted_iota(jnp.int32, (own, fits), 0)
    mine = (lane == row + own * r).astype(F32)

    def rows_of(b):
        return pl.ds(pl.multiple_of(b * block, block), block)

    def back_block(b, vectors):
        left = jnp.transpose(vectors).astype(BF16)
        at = rows_of(b)

        @pl.loop(0, width // wide)
        def _(j):
            cols = pl.ds(pl.multiple_of(j * wide, wide), wide)
            h_ref[:, cols] += jnp.dot(left, design[at, cols], preferred_element_type=F32)

    def reduce_scatter():
        def fits_of(i):
            return pl.ds(pl.multiple_of(i * own, own), own)

        for j in range(chips):
            cs[j] = h_ref[fits_of(2 * j + 1 - core), :].astype(BF16)
        swap = remote(cs, cr, c_send, c_recv, (sibling, c))
        swap.start()
        swap.wait()

        def send(d):
            to = lax.rem(chip + d, chips)
            return remote(rs.at[to], rr.at[chip], r_send.at[to], r_recv.at[chip], (2 * to + core, c))

        def arrived(d):
            frm = lax.rem(chip + d, chips)
            return remote(rs.at[frm], rr.at[frm], r_send.at[frm], r_recv.at[frm], (2 * frm + core, c))

        @pl.loop(1, chips)
        def _(d):
            to = lax.rem(chip + d, chips)
            rs[to] = (h_ref[fits_of(2 * to + core), :] + cr[to].astype(F32)).astype(BF16)
            send(d).start()

        h_ref[fits_of(r), :] += cr[chip].astype(F32)

        @pl.loop(1, chips)
        def _(d):
            arrived(d).wait_recv()
            h_ref[fits_of(r), :] += rr[lax.rem(chip + d, chips)].astype(F32)

        @pl.loop(1, chips)
        def _(d):
            send(d).wait_send()

        return scale_ref[...] * h_ref[fits_of(r), :]

    def squared(g):
        gx[0] = jnp.broadcast_to(jnp.sum(g * g, axis=1, keepdims=True), (own, fits))
        swap = remote(gx.at[0], gx.at[1], g_send, g_recv, partner)
        swap.start()
        swap.wait()
        return gx[0] + gx[1]

    def gather():
        def send(d):
            to = lax.rem(chip + d, chips)
            return remote(sp_all.at[r], sp_all.at[r], a_send.at[to], a_recv.at[r], (2 * to + core, c))

        def relay(d):
            slot = 2 * lax.rem(chip + d, chips) + core
            return remote(sp_all.at[slot], sp_all.at[slot], f_send.at[lax.div(slot, 2)],
                          a_recv.at[slot], (sibling, c))

        def arrived(slot):
            return remote(sp_all.at[slot], sp_all.at[slot], a_send.at[0], a_recv.at[slot], (sibling, c))

        @pl.loop(1, chips)
        def _(d):
            send(d).start()

        relay(0).start()

        @pl.loop(1, chips)
        def _(d):
            arrived(2 * lax.rem(chip + d, chips) + core).wait_recv()
            relay(d).start()

        @pl.loop(0, chips)
        def _(d):
            arrived(2 * lax.rem(chip + d, chips) + 1 - core).wait_recv()

        for j in range(chips):
            pair = jnp.concatenate([sp_all[2 * j].astype(F32), sp_all[2 * j + 1].astype(F32)], axis=0)
            spm[2 * own * j:2 * own * (j + 1), :] = pair.astype(BF16)

        @pl.loop(1, chips)
        def _(d):
            send(d).wait_send()

        @pl.loop(0, chips)
        def _(d):
            relay(d).wait_send()

    def x_copy(b):
        return remote(xs.at[b], xr.at[b], x_send.at[b], x_recv.at[b], partner)

    def forward():
        @pl.loop(0, BLOCKS)
        def _(b):
            part = lax.dot_general(design[rows_of(b), :], spm[...], (((1,), (1,)), ((), ())),
                                   preferred_element_type=F32)
            xs[b] = part.astype(BF16)
            x_copy(b).start()

    def image_block(b, delta):
        x_copy(b).wait_recv()
        image = xs[b].astype(F32) + xr[b].astype(F32)
        img[rows_of(b), :] = image
        return image, delta + jnp.sum(image * image, axis=0, keepdims=True)

    def stat_send(d):
        to = lax.rem(r + d, n)
        return remote(st.at[r], st.at[r], s_send.at[to], s_recv.at[r], (to, c))

    def stats_start(delta):
        st[r] = jnp.concatenate(
            [delta, jnp.sum(gam_ref[...] * mine, axis=0, keepdims=True)], axis=0)

        @pl.loop(1, n)
        def _(d):
            stat_send(d).start()

    def stats_finish():
        @pl.loop(1, n)
        def _(d):
            frm = lax.rem(r + d, n)
            remote(st.at[frm], st.at[frm], s_send.at[frm], s_recv.at[frm], (frm, c)).wait_recv()

        @pl.loop(1, n)
        def _(d):
            stat_send(d).wait_send()

        total = st[0]
        for i in range(1, n):
            total = total + st[i]
        return total[1:2, :] / total[0:1, :]

    def x_done():
        @pl.loop(0, BLOCKS)
        def _(b):
            x_copy(b).wait_send()

    def own_fits(values):
        return jnp.sum(mine * values, axis=1, keepdims=True)

    def publish():
        sp_all[r] = (scale_ref[...] * p_ref[...]).astype(BF16)

    h_ref[...] = jnp.zeros_like(h_ref)
    res_ref[...] = targets_ref[...].astype(F32)
    sol_ref[...] = jnp.zeros_like(sol_ref)
    for b in range(BLOCKS):
        load(b).wait()

    @pl.loop(0, BLOCKS)
    def _(b):
        back_block(b, res_ref[rows_of(b), :])

    pl.semaphore_wait(barrier, n)
    g = reduce_scatter()
    g_ref[...] = g
    p_ref[...] = g
    publish()
    gam_ref[...] = squared(g)

    @pl.loop(0, ITERS - 1)
    def _(step):
        gather()
        forward()
        h_ref[...] = jnp.zeros_like(h_ref)

        def one(b, delta):
            image, delta = image_block(b, delta)
            back_block(b, image)
            return delta

        delta = lax.fori_loop(0, BLOCKS, one, jnp.zeros((1, fits), F32))
        stats_start(delta)
        h = reduce_scatter()
        alpha = stats_finish()
        own_alpha = own_fits(alpha)
        p = p_ref[...]
        sol_ref[...] += own_alpha * p
        g = g_ref[...] - own_alpha * h
        g_ref[...] = g
        gamma_new = squared(g)
        beta = (gamma_new / gam_ref[...])[:, 0:1]
        gam_ref[...] = gamma_new
        p_ref[...] = g + beta * p
        publish()
        x_done()
        res_ref[...] -= alpha * img[...]

    gather()
    forward()
    delta = lax.fori_loop(0, BLOCKS, lambda b, d: image_block(b, d)[1], jnp.zeros((1, fits), F32))
    stats_start(delta)
    alpha = stats_finish()
    sol_ref[...] += own_fits(alpha) * p_ref[...]
    res_ref[...] -= alpha * img[...]
    x_done()


def fused(n, design, targets, col_scale):
    rows, width = design.shape
    fits = targets.shape[1]
    own, chips, block = fits // n, n // 2, rows // BLOCKS
    vmem = pl.BlockSpec(memory_space=pltpu.VMEM)
    dma = pltpu.SemaphoreType.DMA
    sol, res = pl.pallas_call(
        functools.partial(kernel, n),
        out_shape=(jax.ShapeDtypeStruct((own, width), F32),
                   jax.ShapeDtypeStruct((rows, fits), F32)),
        in_specs=[pl.BlockSpec(memory_space=pl.ANY), vmem, vmem],
        out_specs=(vmem, vmem),
        scratch_shapes=[
            pltpu.VMEM((rows, width), BF16),
            pltpu.VMEM((fits, width), F32),
            pltpu.VMEM((rows, fits), F32),
            pltpu.VMEM((fits, width), BF16),
            pltpu.VMEM((n, own, width), BF16),
            pltpu.VMEM((BLOCKS, block, fits), BF16),
            pltpu.VMEM((BLOCKS, block, fits), BF16),
            pltpu.VMEM((chips, own, width), BF16),
            pltpu.VMEM((chips, own, width), BF16),
            pltpu.VMEM((chips, own, width), BF16),
            pltpu.VMEM((chips, own, width), BF16),
            pltpu.VMEM((n, 2, fits), F32),
            pltpu.VMEM((2, own, fits), F32),
            pltpu.VMEM((own, width), F32),
            pltpu.VMEM((own, width), F32),
            pltpu.VMEM((own, fits), F32),
            dma((BLOCKS,)), dma((BLOCKS,)), dma((BLOCKS,)), dma, dma,
            dma((chips,)), dma((chips,)), dma((chips,)), dma((n,)), dma((chips,)),
            dma((n,)), dma((n,)), dma, dma,
        ],
        compiler_params=pltpu.CompilerParams(
            collective_id=0, has_side_effects=True, vmem_limit_bytes=48 * 1024 * 1024),
        name="cg",
    )(design, targets, col_scale[None, :])
    return sol.T, res


def plain(design, targets, col_scale):
    fits = targets.shape[1]
    row_count = lax.axis_size("rows")
    residual = targets.astype(F32)
    scale = col_scale[:, None]

    def gradient_of(vectors):
        local = lax.dot_general(design, vectors, (((0,), (0,)), ((), ())), preferred_element_type=F32)
        return scale * lax.psum(local, "rows")

    def squared(values):
        return lax.psum(jnp.sum(values * values, axis=0), "cols")

    gradient = gradient_of(targets)
    gamma = squared(gradient)
    solution = jnp.zeros(gradient.shape, F32)
    direction = gradient
    for step in range(ITERS):
        scaled_dir = (scale * direction).astype(BF16)
        image = lax.psum(
            jnp.dot(design, scaled_dir, preferred_element_type=F32).astype(BF16), "cols"
        ).astype(F32)
        delta = lax.psum(jnp.sum(image * image, axis=0), "rows")
        alpha = gamma / delta
        solution = solution + alpha * direction
        residual = residual - alpha * image
        if step + 1 < ITERS:
            gradient = gradient_of(residual.astype(BF16))
            gamma_new = squared(gradient)
            direction = gradient + gamma_new / gamma * direction
            gamma = gamma_new
    own = fits // row_count
    part = lax.dynamic_slice_in_dim(solution, lax.axis_index("rows") * own, own, 1)
    return (part, residual)


def solution(mesh):
    n, pair = mesh.shape["rows"], mesh.shape["cols"]

    def per_device(design, targets, col_scale):
        rows, width = design.shape
        fits = targets.shape[1]
        fits_tile = fits % (8 * n) == 0 and fits % 128 == 0
        if pair == 2 and n % 2 == 0 and fits_tile and rows % (BLOCKS * 128) == 0 and width % 128 == 0:
            return fused(n, design, targets, col_scale)
        return plain(design, targets, col_scale)

    in_specs = (P("rows", "cols"), P("rows", None), P("cols"))
    out_specs = (P("cols", "rows"), P("rows", None))
    return jax.shard_map(
        per_device, mesh=mesh, in_specs=in_specs, out_specs=out_specs, check_vma=False
    )
```

```python
import functools

import jax
import jax.numpy as jnp
from jax import lax
from jax.experimental import pallas as pl
from jax.experimental.pallas import tpu as pltpu
from jax.sharding import PartitionSpec as P

ITERS = 6
BLOCKS = 4
F32 = jnp.float32
BF16 = jnp.bfloat16
MESH = pl.DeviceIdType.MESH


def kernel(n, design_hbm, targets_ref, scale_ref, sol_ref, res_ref,
           design, h_ref, img, spm, sp_all, xs, xr, cs, cr, ys, yr, rs, rr, st, gx,
           g_ref, p_ref, gam_ref,
           load_sem, x_send, x_recv, c_send, c_recv, r_send, r_recv,
           a_send, a_recv, b_send, f_send, y_send, y_recv, s_send, s_recv, g_send, g_recv):
    rows, width = design.shape
    fits = targets_ref.shape[1]
    own = fits // n
    chips = n // 2
    block = rows // BLOCKS
    wide = 512 if width % 512 == 0 else width
    r, c = lax.axis_index("rows"), lax.axis_index("cols")
    core, chip = lax.rem(r, 2), lax.div(r, 2)
    sibling = r + 1 - 2 * core
    partner = (r, 1 - c)
    side, place, line = lax.rem(chip, 2), lax.div(chip, 2), chips // 2
    across = (r + 2 - 4 * side, c)
    order = sorted(range(1, line), key=lambda d: -min(d, line - d))

    def place_at(d):
        return lax.rem(place + d, line)

    def remote(src, dst, send, recv, to):
        return pltpu.make_async_remote_copy(
            src_ref=src, dst_ref=dst, send_sem=send, recv_sem=recv,
            device_id=to, device_id_type=MESH)

    def rows_of(b):
        return pl.ds(pl.multiple_of(b * block, block), block)

    def load(b):
        at = rows_of(b)
        return pltpu.make_async_copy(design_hbm.at[at], design.at[at], load_sem.at[b])

    for b in range(BLOCKS):
        load(b).start()
    barrier = pltpu.get_barrier_semaphore()

    @pl.loop(1, n)
    def _(d):
        pl.semaphore_signal(barrier, inc=1, device_id=(lax.rem(r + d, n), c), device_id_type=MESH)

    pl.semaphore_signal(barrier, inc=1, device_id=partner, device_id_type=MESH)

    lane = lax.broadcasted_iota(jnp.int32, (own, fits), 1)
    row = lax.broadcasted_iota(jnp.int32, (own, fits), 0)
    mine = (lane == row + own * r).astype(F32)

    def back_block(b, vectors):
        left = jnp.transpose(vectors).astype(BF16)
        at = rows_of(b)

        @pl.loop(0, width // wide)
        def _(j):
            cols = pl.ds(pl.multiple_of(j * wide, wide), wide)
            h_ref[:, cols] += jnp.dot(left, design[at, cols], preferred_element_type=F32)

    def reduce_scatter():
        def fits_of(i):
            return pl.ds(pl.multiple_of(i * own, own), own)

        def swap(j):
            return remote(cs.at[j], cr.at[j], c_send.at[j], c_recv.at[j], (sibling, c))

        def cross(z):
            return remote(ys.at[z], yr.at[z], y_send.at[z], y_recv.at[z], across)

        def send(z):
            return remote(rs.at[z], rr.at[place], r_send.at[z], r_recv.at[place],
                          (4 * z + 2 * side + core, c))

        def arrived(z):
            return remote(rs.at[z], rr.at[z], r_send.at[z], r_recv.at[z],
                          (4 * z + 2 * side + core, c))

        def chip_sum(j):
            swap(j).wait_recv()
            return h_ref[fits_of(2 * j + core), :] + cr[j].astype(F32)

        for other in (1 - side, side):
            for d in order + [0]:
                j = 2 * place_at(d) + other
                cs[j] = h_ref[fits_of(2 * j + 1 - core), :].astype(BF16)
                swap(j).start()

        for d in order + [0]:
            z = place_at(d)
            ys[z] = chip_sum(2 * z + 1 - side).astype(BF16)
            cross(z).start()

        for d in order:
            z = place_at(d)
            part = chip_sum(2 * z + side)
            cross(z).wait_recv()
            rs[z] = (part + yr[z].astype(F32)).astype(BF16)
            send(z).start()

        total = chip_sum(chip)
        cross(place).wait_recv()
        total = total + yr[place].astype(F32)
        for d in order:
            z = place_at(line - d)
            arrived(z).wait_recv()
            total = total + rr[z].astype(F32)

        @pl.loop(0, chips)
        def _(j):
            swap(j).wait_send()

        for d in order + [0]:
            cross(place_at(d)).wait_send()
        for d in order:
            send(place_at(d)).wait_send()

        return scale_ref[...] * total

    def squared(g):
        gx[0] = jnp.broadcast_to(jnp.sum(g * g, axis=1, keepdims=True), (own, fits))
        swap = remote(gx.at[0], gx.at[1], g_send, g_recv, partner)
        swap.start()
        swap.wait()
        return gx[0] + gx[1]

    def gather():
        def send(z):
            return remote(sp_all.at[r], sp_all.at[r], a_send.at[z], a_recv.at[r],
                          (4 * z + 2 * side + core, c))

        def cross(z):
            slot = 4 * z + 2 * side + core
            return remote(sp_all.at[slot], sp_all.at[slot], b_send.at[z], a_recv.at[slot], across)

        def relay(j):
            slot = 2 * j + core
            return remote(sp_all.at[slot], sp_all.at[slot], f_send.at[j], a_recv.at[slot], (sibling, c))

        def arrived(slot):
            return remote(sp_all.at[slot], sp_all.at[slot], f_send.at[0], a_recv.at[slot], (sibling, c))

        cross(place).start()
        for d in order:
            send(place_at(d)).start()
        relay(chip).start()
        later = [line - d for d in reversed(order)]
        for d in later:
            z = place_at(d)
            arrived(4 * z + 2 * side + core).wait_recv()
            cross(z).start()
            relay(2 * z + side).start()
        for d in [0] + later:
            j = 2 * place_at(d) + 1 - side
            arrived(2 * j + core).wait_recv()
            relay(j).start()
        for other in (side, 1 - side):
            for d in [0] + later:
                j = 2 * place_at(d) + other
                arrived(2 * j + 1 - core).wait_recv()
                pair = jnp.concatenate([sp_all[2 * j].astype(F32), sp_all[2 * j + 1].astype(F32)], axis=0)
                spm[pl.ds(pl.multiple_of(2 * own * j, 2 * own), 2 * own), :] = pair.astype(BF16)

        for d in order:
            send(place_at(d)).wait_send()
        for d in [0] + later:
            cross(place_at(d)).wait_send()

        @pl.loop(0, chips)
        def _(j):
            relay(j).wait_send()

    def x_copy(b):
        return remote(xs.at[b], xr.at[b], x_send.at[b], x_recv.at[b], partner)

    def forward():
        @pl.loop(0, BLOCKS)
        def _(b):
            part = lax.dot_general(design[rows_of(b), :], spm[...], (((1,), (1,)), ((), ())),
                                   preferred_element_type=F32)
            xs[b] = part.astype(BF16)
            x_copy(b).start()

    def image_block(b, delta):
        x_copy(b).wait_recv()
        image = xs[b].astype(F32) + xr[b].astype(F32)
        img[rows_of(b), :] = image
        return image, delta + jnp.sum(image * image, axis=0, keepdims=True)

    def stat_send(d):
        to = lax.rem(r + d, n)
        return remote(st.at[r], st.at[r], s_send.at[to], s_recv.at[r], (to, c))

    def stats_start(delta):
        st[r] = jnp.concatenate(
            [delta, jnp.sum(gam_ref[...] * mine, axis=0, keepdims=True)], axis=0)

        @pl.loop(1, n)
        def _(d):
            stat_send(d).start()

    def stats_finish():
        @pl.loop(1, n)
        def _(d):
            frm = lax.rem(r + d, n)
            remote(st.at[frm], st.at[frm], s_send.at[frm], s_recv.at[frm], (frm, c)).wait_recv()

        @pl.loop(1, n)
        def _(d):
            stat_send(d).wait_send()

        total = st[0]
        for i in range(1, n):
            total = total + st[i]
        return total[1:2, :] / total[0:1, :]

    def x_done():
        @pl.loop(0, BLOCKS)
        def _(b):
            x_copy(b).wait_send()

    def own_fits(values):
        return jnp.sum(mine * values, axis=1, keepdims=True)

    def publish():
        sp_all[r] = (scale_ref[...] * p_ref[...]).astype(BF16)

    h_ref[...] = jnp.zeros_like(h_ref)
    res_ref[...] = targets_ref[...].astype(F32)
    sol_ref[...] = jnp.zeros_like(sol_ref)
    @pl.loop(0, BLOCKS)
    def _(b):
        load(b).wait()
        back_block(b, res_ref[rows_of(b), :])

    pl.semaphore_wait(barrier, n)
    g = reduce_scatter()
    g_ref[...] = g
    p_ref[...] = g
    publish()
    gam_ref[...] = squared(g)

    @pl.loop(0, ITERS - 1)
    def _(step):
        gather()
        forward()
        h_ref[...] = jnp.zeros_like(h_ref)

        def one(b, delta):
            image, delta = image_block(b, delta)
            back_block(b, image)
            return delta

        delta = lax.fori_loop(0, BLOCKS, one, jnp.zeros((1, fits), F32))
        stats_start(delta)
        h = reduce_scatter()
        alpha = stats_finish()
        own_alpha = own_fits(alpha)
        p = p_ref[...]
        sol_ref[...] += own_alpha * p
        g = g_ref[...] - own_alpha * h
        g_ref[...] = g
        gamma_new = squared(g)
        beta = (gamma_new / gam_ref[...])[:, 0:1]
        gam_ref[...] = gamma_new
        p_ref[...] = g + beta * p
        publish()
        x_done()
        res_ref[...] -= alpha * img[...]

    gather()
    forward()
    delta = lax.fori_loop(0, BLOCKS, lambda b, d: image_block(b, d)[1], jnp.zeros((1, fits), F32))
    stats_start(delta)
    alpha = stats_finish()
    sol_ref[...] += own_fits(alpha) * p_ref[...]
    res_ref[...] -= alpha * img[...]
    x_done()


def fused(n, design, targets, col_scale):
    rows, width = design.shape
    fits = targets.shape[1]
    own, chips, line, block = fits // n, n // 2, n // 4, rows // BLOCKS
    vmem = pl.BlockSpec(memory_space=pltpu.VMEM)
    dma = pltpu.SemaphoreType.DMA
    sol, res = pl.pallas_call(
        functools.partial(kernel, n),
        out_shape=(jax.ShapeDtypeStruct((own, width), F32),
                   jax.ShapeDtypeStruct((rows, fits), F32)),
        in_specs=[pl.BlockSpec(memory_space=pl.ANY), vmem, vmem],
        out_specs=(vmem, vmem),
        scratch_shapes=[
            pltpu.VMEM((rows, width), BF16),
            pltpu.VMEM((fits, width), F32),
            pltpu.VMEM((rows, fits), F32),
            pltpu.VMEM((fits, width), BF16),
            pltpu.VMEM((n, own, width), BF16),
            pltpu.VMEM((BLOCKS, block, fits), BF16),
            pltpu.VMEM((BLOCKS, block, fits), BF16),
            pltpu.VMEM((chips, own, width), BF16),
            pltpu.VMEM((chips, own, width), BF16),
            pltpu.VMEM((line, own, width), BF16),
            pltpu.VMEM((line, own, width), BF16),
            pltpu.VMEM((line, own, width), BF16),
            pltpu.VMEM((line, own, width), BF16),
            pltpu.VMEM((n, 2, fits), F32),
            pltpu.VMEM((2, own, fits), F32),
            pltpu.VMEM((own, width), F32),
            pltpu.VMEM((own, width), F32),
            pltpu.VMEM((own, fits), F32),
            dma((BLOCKS,)), dma((BLOCKS,)), dma((BLOCKS,)), dma((chips,)), dma((chips,)),
            dma((line,)), dma((line,)), dma((line,)), dma((n,)), dma((line,)), dma((chips,)),
            dma((line,)), dma((line,)),
            dma((n,)), dma((n,)), dma, dma,
        ],
        compiler_params=pltpu.CompilerParams(
            collective_id=0, has_side_effects=True, vmem_limit_bytes=48 * 1024 * 1024),
        name="cg",
    )(design, targets, col_scale[None, :])
    return sol.T, res


def plain(design, targets, col_scale):
    fits = targets.shape[1]
    row_count = lax.axis_size("rows")
    residual = targets.astype(F32)
    scale = col_scale[:, None]

    def gradient_of(vectors):
        local = lax.dot_general(design, vectors, (((0,), (0,)), ((), ())), preferred_element_type=F32)
        return scale * lax.psum(local, "rows")

    def squared(values):
        return lax.psum(jnp.sum(values * values, axis=0), "cols")

    gradient = gradient_of(targets)
    gamma = squared(gradient)
    solution = jnp.zeros(gradient.shape, F32)
    direction = gradient
    for step in range(ITERS):
        scaled_dir = (scale * direction).astype(BF16)
        image = lax.psum(
            jnp.dot(design, scaled_dir, preferred_element_type=F32).astype(BF16), "cols"
        ).astype(F32)
        delta = lax.psum(jnp.sum(image * image, axis=0), "rows")
        alpha = gamma / delta
        solution = solution + alpha * direction
        residual = residual - alpha * image
        if step + 1 < ITERS:
            gradient = gradient_of(residual.astype(BF16))
            gamma_new = squared(gradient)
            direction = gradient + gamma_new / gamma * direction
            gamma = gamma_new
    own = fits // row_count
    part = lax.dynamic_slice_in_dim(solution, lax.axis_index("rows") * own, own, 1)
    return (part, residual)


def solution(mesh):
    n, pair = mesh.shape["rows"], mesh.shape["cols"]

    def per_device(design, targets, col_scale):
        rows, width = design.shape
        fits = targets.shape[1]
        fits_tile = fits % (8 * n) == 0 and fits % 128 == 0
        if pair == 2 and n % 4 == 0 and fits_tile and rows % (BLOCKS * 128) == 0 and width % 128 == 0:
            return fused(n, design, targets, col_scale)
        return plain(design, targets, col_scale)

    in_specs = (P("rows", "cols"), P("rows", None), P("cols"))
    out_specs = (P("cols", "rows"), P("rows", None))
    return jax.shard_map(
        per_device, mesh=mesh, in_specs=in_specs, out_specs=out_specs, check_vma=False
    )
```
